32 devices in a mesh: groups: 2 (over x), samp: 16 (over z, y, core).
Axes of the slice: x: 2, y: 2, z: 4, core: 2. Of those that a mesh axis runs over, the one named last changes fastest.
Arguments:
- dosage: bfloat16 [8192, 8192], P(('groups', 'samp')), parts along dimension 0, may hold values from 0 to 2
- covariates: bfloat16 [8192, 96], P(('groups', 'samp')), parts along dimension 0, may hold values from -8 to 8
- expression: bfloat16 [8192, 8192], P('groups', 'samp'), parts along dimension 0, may hold values from -10 to 10
- block_index: int32 [4, 1024], P('groups'), parts along dimension 0, may hold values from 0 to 8191
- expr_row: int32 [8192], P('groups'), parts along dimension 0, may hold values from 0 to 4095, each once
Outputs:
- zscore: float32 [4096, 8192], P('groups', 'samp'), parts along dimension 0
The draws below stay inside these ranges and needn't reach their ends.
There are 2 independent parts, one for each index of `groups`. The reference program is written for one: setup_inputs(seed, part) draws one part's arguments, and reference() takes and returns one part's arrays. A program takes and returns all parts, laid end to end along the dimension named above; each array names one. Nothing has to cross between parts.
Inputs may be any that keep to these rules, and one draw needn't show every extreme that they name: `expr_row`: every expression row appears once.
All inputs are finite; a program needn't handle non-finite values.
Results may differ from the reference program's by a relative error of at most 0.0029.
Values may be sent and summed in bfloat16 or wider, within the bound.
A program may use at most 192 MiB of HBM per device.

```python
import math
import jax
import jax.numpy as jnp
from jax import lax

K = 96
V = 1024
BLOCKS = 2
VPANEL = 8192
NSAMP = 4096
GENES = 8192


def covariate_base(key):
    first = jax.random.fold_in(key, 11)
    normal_part = jax.random.normal(first, (NSAMP, K), jnp.float32)
    rising = 1.0 + 2.0 * jnp.arange(NSAMP, dtype=jnp.float32) / NSAMP
    return jnp.clip(normal_part * rising[:, None], -8.0, 8.0)


def draw_covariates(key, part):
    return covariate_base(key).astype(jnp.bfloat16)


def draw_dosage(key, part):
    base = covariate_base(key)
    loading = jax.random.normal(jax.random.fold_in(key, 21), (K, VPANEL), jnp.float32)
    noise_key = jax.random.fold_in(key, 22)
    noise = jax.random.uniform(noise_key, (NSAMP, VPANEL), jnp.float32, -0.6, 0.6)
    shared = jnp.dot(base, loading) * (0.3 / K ** 0.5)
    return jnp.clip(1.0 + shared + noise, 0.0, 2.0).astype(jnp.bfloat16)


def draw_expression(key, part):
    base = covariate_base(key)
    loading = jax.random.normal(jax.random.fold_in(key, 31), (K, GENES), jnp.float32)
    noise_key = jax.random.fold_in(key, 32)
    noise = jax.random.normal(noise_key, (NSAMP, GENES), jnp.float32)
    shared = jnp.dot(base, loading) * (0.5 / K ** 0.5)
    return jnp.clip(shared + noise, -10.0, 10.0).astype(jnp.bfloat16)


def plant(entries, own_key, least, high):
    place = [jax.random.randint(jax.random.fold_in(own_key, axis), (), 0, length) for axis, length in enumerate(entries.shape)]
    widest = entries.shape.index(max(entries.shape))
    beside = place[:widest] + [(place[widest] + 1) % entries.shape[widest]] + place[widest + 1:]
    return entries.at[tuple(place)].set(least).at[tuple(beside)].set(high)


def setup_inputs(seed: int = 0, part: int = 0) -> dict:
    key_list = jax.random.split(jax.random.key(seed), 6)
    part_keys = jax.random.split(jax.random.fold_in(key_list[5], part), 6)
    dosage = draw_dosage(jax.random.fold_in(jax.random.fold_in(key_list[5], part), 71), part)
    covariates = draw_covariates(jax.random.fold_in(jax.random.fold_in(key_list[5], part), 71), part)
    expression = draw_expression(jax.random.fold_in(jax.random.fold_in(key_list[5], part), 71), part)
    block_index = plant(jax.random.randint(part_keys[3], (BLOCKS, V), 0, VPANEL), jax.random.fold_in(part_keys[3], 1), 0, VPANEL - 1).astype(jnp.int32)
    expr_row = jax.random.permutation(part_keys[4], NSAMP).astype(jnp.int32)
    return dict(dosage=dosage, covariates=covariates, expression=expression, block_index=block_index, expr_row=expr_row)


epsilon = 1e-06

def reference(dosage, covariates, expression, block_index, expr_row):
    gram = jnp.dot(covariates.T.astype(jnp.float32), covariates.astype(jnp.float32), preferred_element_type=jnp.float32)
    factor = jnp.linalg.cholesky(gram)
    matched = jnp.take(expression, expr_row, axis=0)
    panel_norm = lax.optimization_barrier(jnp.sum(jnp.square(expression.astype(jnp.float32)), axis=0))
    cov_float = covariates.astype(jnp.float32)
    scale = math.sqrt(NSAMP - K - 1)
    results = []
    for block in range(BLOCKS):
        picked = jnp.take(dosage, block_index[block], axis=1)
        loads = jnp.dot(covariates.T.astype(jnp.float32), picked.astype(jnp.float32), preferred_element_type=jnp.float32)
        coeffs = jax.scipy.linalg.cho_solve((factor, True), loads)
        fitted = jnp.dot(cov_float, coeffs, precision=lax.Precision.HIGHEST)
        resid = (picked.astype(jnp.float32) - fitted).astype(jnp.bfloat16)
        resid_norm = lax.optimization_barrier(jnp.sum(jnp.square(resid.astype(jnp.float32)), axis=0))
        products = jnp.dot(resid.T.astype(jnp.float32), matched.astype(jnp.float32), preferred_element_type=jnp.float32)
        results.append(scale * products * lax.rsqrt(resid_norm + epsilon)[:, None] * lax.rsqrt(panel_norm + epsilon)[None, :])
    return jnp.concatenate(results, axis=0)
```

```python
import functools
import math

import jax
import jax.numpy as jnp
from jax import lax
from jax.experimental import pallas as pl
from jax.experimental.pallas import tpu as pltpu
from jax.sharding import PartitionSpec as P

epsilon = 1e-06
MESH = pl.DeviceIdType.MESH
CHUNKS = 8
SPAN = 1024
COLUMNS = (((1,), (1,)), ((), ()))


def terms(x):
    first = x.astype(jnp.bfloat16)
    rest = x - first.astype(jnp.float32)
    second = rest.astype(jnp.bfloat16)
    return [first, second, (rest - second.astype(jnp.float32)).astype(jnp.bfloat16)]


def exchange(n, scale, dosage, c_ref, expr, index_ref, row_ref, out_ref,
             panel, covs, mine, theirs, picked, turned, raw, lines, rows_f32, ebuf,
             norm, norm_other, part, gram, right, lower, lower_scaled, parts, sq,
             result, load_sem, expr_sem, send_sem, recv_sem, core_sem):
    depth = n // 4
    me = lax.axis_index("samp")
    z, y, core = me // 4, (me // 2) % 2, me % 2
    group = lax.axis_index("groups")
    here = picked.shape[1]
    variants = picked.shape[0]
    half = panel.shape[0]
    samples = panel.shape[1]
    genes = mine.shape[1]
    covars = covs.shape[0]
    block_width = index_ref.shape[1]
    width = half // CHUNKS
    pieces = CHUNKS + 1
    pair = 2 * here
    top, bottom = depth - 1, 0
    balance = depth >= 4

    def device(zz, yy, cc):
        return (group, (zz * 2 + yy) * 2 + cc)

    partner = device(z, y, 1 - core)
    below, above = z > bottom, z < top

    panel_width = dosage.shape[1]
    quarters = raw.shape[0]
    quarter = panel_width // quarters

    def loading(q):
        return pltpu.make_async_copy(
            dosage.at[:, pl.ds(q * quarter, quarter)], raw.at[q], load_sem.at[q])

    for q in range(quarters):
        loading(q).start()

    barrier = pltpu.get_barrier_semaphore()
    pl.semaphore_signal(barrier, inc=1, device_id=partner, device_id_type=MESH)
    for h in range(2):
        pl.semaphore_signal(barrier, inc=1, device_id=device(z, 1 - y, h), device_id_type=MESH)

        @pl.when(below)
        def _():
            pl.semaphore_signal(barrier, inc=1, device_id=device(z - 1, y, h), device_id_type=MESH)

        @pl.when(above)
        def _():
            pl.semaphore_signal(barrier, inc=1, device_id=device(z + 1, y, h), device_id_type=MESH)

    def chip(zz, yy):
        return zz * 2 + yy

    def stripe(c):
        return pl.ds(pl.multiple_of(c * pair, pair), pair)

    def single(zz, yy, cc):
        return pl.ds(pl.multiple_of(((zz * 2 + yy) * 2 + cc) * here, here), here)

    def row_range(piece):
        return pl.ds((piece - 1) * width, width)

    def block(piece, where):
        if piece == 0:
            return covs.at[:, where]
        return panel.at[row_range(piece), where]

    def own(piece, h):
        if piece == 0:
            return c_ref
        start = h * half + (piece - 1) * width
        if not isinstance(h, int):
            start = pl.multiple_of(start, width)
        return picked.at[pl.ds(start, width), :]

    started = []

    def send(when, src, dst, target, recv):
        copy = pltpu.make_async_remote_copy(
            src_ref=src, dst_ref=dst, send_sem=send_sem.at[len(started)], recv_sem=recv,
            device_id=target, device_id_type=MESH)
        if when is None:
            copy.start()
        else:
            pl.when(when)(copy.start)
        started.append((when, copy))

    def send_own(piece):
        where = single(z, y, core)
        sem = recv_sem.at[piece, chip(z, y)]
        for h in range(2):
            src = own(piece, h)
            dst = block(piece, where)
            send(None, src, dst, device(z, 1 - y, h), sem)
            send(below, src, dst, device(z - 1, y, h), sem)
            send(above, src, dst, device(z + 1, y, h), sem)
        send(None, own(piece, 1 - core), block(piece, where), partner, sem)
        if piece == 0:
            covs[:, where] = c_ref[...]
        else:
            start = pl.multiple_of(core * half + (piece - 1) * width, width)
            panel[row_range(piece), where] = picked[pl.ds(start, width), :]

    def arrive(piece, zz, yy):
        where = stripe(chip(zz, yy))
        pltpu.make_async_remote_copy(
            src_ref=block(piece, where), dst_ref=block(piece, where), send_sem=send_sem.at[0],
            recv_sem=recv_sem.at[piece, chip(zz, yy)], device_id=partner,
            device_id_type=MESH).wait_recv()

    def arrive_partner(piece):
        where = single(z, y, 1 - core)
        pltpu.make_async_remote_copy(
            src_ref=block(piece, where), dst_ref=block(piece, where), send_sem=send_sem.at[0],
            recv_sem=recv_sem.at[piece, chip(z, y)], device_id=partner,
            device_id_type=MESH).wait_recv()

    def forward(when, piece, zz, yy, target):
        where = block(piece, stripe(chip(zz, yy)))
        send(when, where, where, target, recv_sem.at[piece, chip(zz, yy)])

    down = device(z - 1, y, core)
    up = device(z + 1, y, core)
    across = device(z, 1 - y, core)

    def relay_cross(piece):
        arrive(piece, z, 1 - y)
        if balance:
            low, high = z == bottom, z == top
            if piece % 2:
                low_too, high_too = z == top - 1, z == bottom + 1
                forward(low | low_too, piece, z, 1 - y, up)
                forward(high | high_too, piece, z, 1 - y, down)
            else:
                forward(low, piece, z, 1 - y, up)
                forward(high, piece, z, 1 - y, down)

    def relay(piece, d):
        for sign in (1, -1):
            src = z + sign * d
            valid = (src <= top) if sign > 0 else (src >= bottom)
            onward = below if sign > 0 else above
            target = down if sign > 0 else up

            @pl.when(valid)
            def _():
                arrive(piece, src, y)

            forward(valid & onward, piece, src, y, target)
            cross = valid
            if balance and d == 1:
                end = (z == top - 1) if sign > 0 else (z == bottom + 1)
                cross = cross & jnp.logical_not(end)
                if piece % 2:
                    edge = (z == bottom) if sign > 0 else (z == top)
                    cross = cross & jnp.logical_not(edge)
            forward(cross, piece, src, y, across)

    def settle(piece):
        arrive_partner(piece)
        for d in range(1, depth):
            for sign in (1, -1):
                src = z + sign * d

                @pl.when((src <= top) if sign > 0 else (src >= bottom))
                def _():
                    arrive(piece, src, 1 - y)

    block_lanes = 512

    def turn(q):
        def body(i, _):
            lanes = pl.ds(pl.multiple_of(i * block_lanes, block_lanes), block_lanes)
            x = raw[q, :, lanes].astype(jnp.float32)
            rows = pl.ds(pl.multiple_of(q * quarter + i * block_lanes, block_lanes), block_lanes)
            turned[rows, :] = x.T
            return 0

        lax.fori_loop(0, quarter // block_lanes, body, 0)

    batch = lines.shape[0]

    def pick(piece):
        for h in range(2):
            first = h * half + (piece - 1) * width

            def body(i, _):
                base = first + i * batch
                b, at = base // block_width, lax.rem(base, block_width)
                for u in range(batch):
                    lines[pl.ds(u, 1), :] = turned[pl.ds(index_ref[b, at + u], 1), :]
                picked[pl.ds(pl.multiple_of(base, batch), batch), :] = (
                    lines[...].astype(jnp.bfloat16))
                return 0

            lax.fori_loop(0, width // batch, body, 0)

    lanes = here
    expr_parts = genes // lanes

    def loading_expr(p):
        return pltpu.make_async_copy(expr.at[:, pl.ds(p * lanes, lanes)], ebuf, expr_sem)

    def widen(p):
        loading_expr(p).wait()
        columns = slice(p * lanes, (p + 1) * lanes)
        step = samples // 16

        def body(i, total):
            rows = pl.ds(pl.multiple_of(i * step, step), step)
            x = ebuf[rows, :].astype(jnp.float32)
            turned[rows, :] = x
            return total + jnp.sum(x * x, axis=0, keepdims=True)

        total = lax.fori_loop(0, 16, body, jnp.zeros((1, lanes), jnp.float32))
        norm[:, columns] = jnp.broadcast_to(total, (8, lanes))
        if p + 1 < expr_parts:
            loading_expr(p + 1).start()
        else:
            send(None, norm, norm_other, partner, core_sem.at[0])

    match_parts = 4

    def match(p, q):
        columns = slice(p * lanes, (p + 1) * lanes)
        span = samples // match_parts

        def body(i, _):
            base = q * span + i * batch
            for u in range(batch):
                lines[pl.ds(u, 1), :] = turned[pl.ds(row_ref[base + u], 1), :]
            mine[pl.ds(pl.multiple_of(base, batch), batch), columns] = (
                lines[...].astype(jnp.bfloat16))
            return 0

        lax.fori_loop(0, span // batch, body, 0)

    def send_match(p, q):
        span = samples // match_parts
        where = (pl.ds(q * span, span), pl.ds(p * lanes, lanes))
        send(None, mine.at[where], theirs.at[where], partner,
             core_sem.at[1 + p * match_parts + q])

    def arrive_match():
        pltpu.make_async_remote_copy(
            src_ref=norm, dst_ref=norm_other, send_sem=send_sem.at[0],
            recv_sem=core_sem.at[0], device_id=partner, device_id_type=MESH).wait_recv()
        span = samples // match_parts
        for p in range(expr_parts):
            for q in range(match_parts):
                where = (pl.ds(q * span, span), pl.ds(p * lanes, lanes))
                pltpu.make_async_remote_copy(
                    src_ref=mine.at[where], dst_ref=theirs.at[where], send_sem=send_sem.at[0],
                    recv_sem=core_sem.at[1 + p * match_parts + q], device_id=partner,
                    device_id_type=MESH).wait_recv()

    span = min(SPAN, samples)
    spans = samples // span

    def cut(j):
        return pl.ds(pl.multiple_of(j * span, span), span)

    def make_gram():
        settle(0)
        gram[...] = jnp.zeros_like(gram)

        def add(j, _):
            c = covs[:, cut(j)]
            gram[...] += lax.dot_general(c, c, COLUMNS, preferred_element_type=jnp.float32)
            return 0

        lax.fori_loop(0, spans, add, 0)
        row = lax.broadcasted_iota(jnp.int32, (covars, covars), 0)
        lane = lax.broadcasted_iota(jnp.int32, (covars, covars), 1)
        right[...] = (row == lane).astype(jnp.float32)

    def eliminate(low, high):
        lane = lax.broadcasted_iota(jnp.int32, (covars, covars), 1)
        first_lane = lax.broadcasted_iota(jnp.int32, (1, covars), 1)
        first_row = lax.broadcasted_iota(jnp.int32, (covars, 1), 0)

        def body(i, _):
            g_row, r_row = gram[pl.ds(i, 1), :], right[pl.ds(i, 1), :]
            pivot = jnp.sum(jnp.where(first_lane == i, g_row, 0.0), axis=1, keepdims=True)
            g = gram[...]
            column = jnp.sum(jnp.where(lane == i, g, 0.0), axis=1, keepdims=True)
            factor = jnp.where(first_row > i, column / pivot, 0.0)
            lower[pl.ds(i, 1), :] = r_row
            lower_scaled[pl.ds(i, 1), :] = r_row / pivot
            gram[...] = g - factor * g_row
            right[...] = right[...] - factor * r_row
            return 0

        lax.fori_loop(low, high, body, 0)

    def solve(piece):
        settle(piece)
        rows = row_range(piece)

        def load(j, total):
            return total + lax.dot_general(
                panel[rows, cut(j)], covs[:, cut(j)], COLUMNS,
                preferred_element_type=jnp.float32)

        loads = lax.fori_loop(0, spans, load, jnp.zeros((width, covars), jnp.float32))
        solved = lax.dot_general(loads, lower[...], COLUMNS, precision=lax.Precision.HIGHEST,
                                 preferred_element_type=jnp.float32)
        coeffs = jnp.dot(solved, lower_scaled[...], precision=lax.Precision.HIGHEST,
                         preferred_element_type=jnp.float32)
        parts[...] = jnp.concatenate(terms(coeffs), axis=1)
        sq[...] = jnp.zeros_like(sq)

    def product(piece, j):
        rows = row_range(piece)
        c = covs[:, cut(j)]
        fitted = jnp.dot(parts[...], jnp.concatenate([c, c, c], axis=0),
                         preferred_element_type=jnp.float32)
        resid = (panel[rows, cut(j)].astype(jnp.float32) - fitted).astype(jnp.bfloat16)
        wide = resid.astype(jnp.float32)
        sq[...] += jnp.sum(wide * wide, axis=1, keepdims=True)
        kept = jnp.dot(resid, mine[cut(j), :], preferred_element_type=jnp.float32)
        given = jnp.dot(resid, theirs[cut(j), :], preferred_element_type=jnp.float32)
        if j == 0:
            result[rows, :] = kept
            part[rows, :] = given
        else:
            result[rows, :] += kept
            part[rows, :] += given

    def out_rows(piece):
        return pl.ds(pl.multiple_of(core * half + (piece - 1) * width, width), width)

    def finish(piece):
        rows = row_range(piece)
        size = scale * lax.rsqrt(sq[...] + epsilon)
        part[rows, :] = part[rows, :] * size * lax.rsqrt(norm_other[:1, :] + epsilon)
        out_ref[out_rows(piece), :] = result[rows, :] * size * lax.rsqrt(norm[:1, :] + epsilon)

    def give(piece):
        send(None, part.at[row_range(piece), :], out_ref.at[out_rows(piece), :], partner,
             core_sem.at[1 + expr_parts * match_parts + piece - 1])

    def receive(piece):
        rows = pl.ds(pl.multiple_of((1 - core) * half + (piece - 1) * width, width), width)
        pltpu.make_async_remote_copy(
            src_ref=part.at[row_range(piece), :], dst_ref=out_ref.at[rows, :],
            send_sem=send_sem.at[0],
            recv_sem=core_sem.at[1 + expr_parts * match_parts + piece - 1], device_id=partner,
            device_id_type=MESH).wait_recv()

    work = []

    def todo(earliest, weight, call, *args):
        work.append((earliest, weight, functools.partial(call, *args)))

    for piece in range(3, pieces):
        todo(0, 0.6, pick, piece)
    sent = None
    for p in range(expr_parts):
        todo(0, 1.0, widen, p)
        for q in range(match_parts):
            todo(0, 1.3, match, p, q)
            if sent is not None:
                todo(0, 0.0, send_match, *sent)
            sent = (p, q)
    todo(0, 0.0, send_match, *sent)
    todo(1, 0.7, make_gram)
    step = covars // 12
    for i in range(12):
        todo(1, 1.2, eliminate, i * step, covars if i == 11 else (i + 1) * step)
    todo(1, 0.0, arrive_match)
    for piece in range(1, pieces):
        todo(piece + 1, 0.6, solve, piece)
        for j in range(spans):
            todo(piece + 1, 0.5, product, piece, j)
        todo(piece + 1, 0.3, finish, piece)
        todo(piece + 1, 0.0, give, piece)

    pl.semaphore_wait(barrier, 3 + 2 * below.astype(jnp.int32) + 2 * above.astype(jnp.int32))
    send_own(0)
    for q in range(quarters):
        loading(q).wait()
        turn(q)
    loading_expr(0).start()
    pick(1)
    pick(2)
    send_own(1)
    slots = depth

    for piece in range(pieces):
        if 0 < piece and piece + 1 < pieces:
            send_own(piece + 1)
        left = sum(w for e, w, _ in work if e <= pieces - 1)
        quota = left / (pieces - piece) / slots

        def run():
            spent = 0.0
            while work and work[0][0] <= piece and (spent < quota or work[0][1] == 0.0):
                spent += work[0][1]
                work.pop(0)[2]()

        relay_cross(piece)
        run()
        for d in range(1, depth):
            relay(piece, d)
            run()
    for _, _, call in work:
        call()
    for piece in range(1, pieces):
        receive(piece)
    for when, copy in started:
        if when is None:
            copy.wait_send()
        else:
            pl.when(when)(copy.wait_send)


def local(n, dosage, covariates, expression, block_index, expr_row):
    blocks, block_width = block_index.shape
    here, covars = covariates.shape
    samples, genes = expression.shape
    variants = blocks * block_width
    half = variants // 2
    width = half // CHUNKS
    scale = math.sqrt(samples - covars - 1)
    vmem = pl.BlockSpec(memory_space=pltpu.VMEM)
    smem = pl.BlockSpec(memory_space=pltpu.SMEM)
    hbm = pl.BlockSpec(memory_space=pl.ANY)
    depth = n // 4
    pieces = CHUNKS + 1
    sends = pieces * (7 + 2 + 4 * (depth - 1)) + 64
    square = pltpu.VMEM((covars, covars), jnp.float32)
    quarters = 4
    return pl.pallas_call(
        functools.partial(exchange, n, scale),
        out_shape=jax.ShapeDtypeStruct((variants, genes), jnp.float32),
        in_specs=[hbm, vmem, hbm, smem, smem],
        out_specs=vmem,
        scratch_shapes=[
            pltpu.VMEM((half, samples), jnp.bfloat16),
            pltpu.VMEM((covars, samples), jnp.bfloat16),
            pltpu.VMEM((samples, genes), jnp.bfloat16),
            pltpu.VMEM((samples, genes), jnp.bfloat16),
            pltpu.VMEM((variants, here), jnp.bfloat16),
            pltpu.VMEM((max(dosage.shape[1], samples), here), jnp.float32),
            pltpu.VMEM((quarters, here, dosage.shape[1] // quarters), jnp.bfloat16),
            pltpu.VMEM((64, here), jnp.float32),
            pltpu.VMEM((8, 128), jnp.float32),
            pltpu.VMEM((samples, here), jnp.bfloat16),
            pltpu.VMEM((8, genes), jnp.float32),
            pltpu.VMEM((8, genes), jnp.float32),
            pltpu.VMEM((half, genes), jnp.float32),
            square, square, square, square,
            pltpu.VMEM((width, 3 * covars), jnp.bfloat16),
            pltpu.VMEM((width, 1), jnp.float32),
            pltpu.VMEM((half, genes), jnp.float32),
            pltpu.SemaphoreType.DMA((quarters,)),
            pltpu.SemaphoreType.DMA,
            pltpu.SemaphoreType.DMA((sends,)),
            pltpu.SemaphoreType.DMA((pieces, n // 2)),
            pltpu.SemaphoreType.DMA((64,)),
        ],
        compiler_params=pltpu.CompilerParams(
            collective_id=0, has_side_effects=True, vmem_limit_bytes=63 * 2**20),
    )(dosage, covariates.T, expression, block_index, expr_row)


def solution(mesh):
    placed = (
        P(("groups", "samp"), None),
        P(("groups", "samp"), None),
        P("groups", "samp"),
        P("groups", None),
        P("groups"),
    )
    return jax.shard_map(
        functools.partial(local, mesh.shape["samp"]),
        mesh=mesh, in_specs=placed, out_specs=P("groups", "samp"), check_vma=False
    )
```

```python
import functools
import math

import jax
import jax.numpy as jnp
from jax import lax
from jax.experimental import pallas as pl
from jax.experimental.pallas import tpu as pltpu
from jax.sharding import PartitionSpec as P

epsilon = 1e-06
MESH = pl.DeviceIdType.MESH
PATTERN = (1, 1, 1, 1, 1, 1, 1, 1)
SPAN = 1024
COLUMNS = (((1,), (1,)), ((), ()))


def terms(x):
    first = x.astype(jnp.bfloat16)
    rest = x - first.astype(jnp.float32)
    second = rest.astype(jnp.bfloat16)
    return [first, second, (rest - second.astype(jnp.float32)).astype(jnp.bfloat16)]


def exchange(n, scale, dosage, c_ref, expr, index_ref, row_ref, out_ref,
             panel, covs, mine, theirs, picked, turned, raw, lines, rows_f32, ebuf,
             norm, norm_other, part, gram, right, lower, lower_scaled, parts, sq,
             result, load_sem, expr_sem, send_sem, recv_sem, core_sem):
    depth = n // 4
    me = lax.axis_index("samp")
    z, y, core = me // 4, (me // 2) % 2, me % 2
    group = lax.axis_index("groups")
    here = picked.shape[1]
    variants = picked.shape[0]
    half = panel.shape[0]
    samples = panel.shape[1]
    genes = mine.shape[1]
    covars = covs.shape[0]
    block_width = index_ref.shape[1]
    widths = [p * half // sum(PATTERN) for p in PATTERN]
    starts = [sum(widths[:k]) for k in range(len(widths))]
    pieces = len(widths) + 1
    pair = 2 * here
    top, bottom = depth - 1, 0
    balance = depth >= 4

    def device(zz, yy, cc):
        return (group, (zz * 2 + yy) * 2 + cc)

    partner = device(z, y, 1 - core)
    below, above = z > bottom, z < top

    panel_width = dosage.shape[1]
    quarters = raw.shape[0]
    quarter = panel_width // quarters

    def loading(q):
        return pltpu.make_async_copy(
            dosage.at[:, pl.ds(q * quarter, quarter)], raw.at[q], load_sem.at[q])

    for q in range(quarters):
        loading(q).start()

    barrier = pltpu.get_barrier_semaphore()
    pl.semaphore_signal(barrier, inc=1, device_id=partner, device_id_type=MESH)
    for h in range(2):
        pl.semaphore_signal(barrier, inc=1, device_id=device(z, 1 - y, h), device_id_type=MESH)

        @pl.when(below)
        def _():
            pl.semaphore_signal(barrier, inc=1, device_id=device(z - 1, y, h), device_id_type=MESH)

        @pl.when(above)
        def _():
            pl.semaphore_signal(barrier, inc=1, device_id=device(z + 1, y, h), device_id_type=MESH)

    def chip(zz, yy):
        return zz * 2 + yy

    def stripe(c):
        return pl.ds(pl.multiple_of(c * pair, pair), pair)

    def single(zz, yy, cc):
        return pl.ds(pl.multiple_of(((zz * 2 + yy) * 2 + cc) * here, here), here)

    def row_range(piece):
        return pl.ds(starts[piece - 1], widths[piece - 1])

    def block(piece, where):
        if piece == 0:
            return covs.at[:, where]
        return panel.at[row_range(piece), where]

    def own(piece, h):
        if piece == 0:
            return c_ref
        start = h * half + starts[piece - 1]
        if not isinstance(h, int):
            start = pl.multiple_of(start, 16)
        return picked.at[pl.ds(start, widths[piece - 1]), :]

    started = []

    def send(when, src, dst, target, recv):
        copy = pltpu.make_async_remote_copy(
            src_ref=src, dst_ref=dst, send_sem=send_sem.at[len(started)], recv_sem=recv,
            device_id=target, device_id_type=MESH)
        if when is None:
            copy.start()
        else:
            pl.when(when)(copy.start)
        started.append((when, copy))

    def send_own(piece):
        where = single(z, y, core)
        sem = recv_sem.at[piece, chip(z, y)]
        for h in range(2):
            src = own(piece, h)
            dst = block(piece, where)
            send(None, src, dst, device(z, 1 - y, h), sem)
            send(below, src, dst, device(z - 1, y, h), sem)
            send(above, src, dst, device(z + 1, y, h), sem)
        send(None, own(piece, 1 - core), block(piece, where), partner, sem)
        if piece == 0:
            covs[:, where] = c_ref[...]
        else:
            start = pl.multiple_of(core * half + starts[piece - 1], 16)
            panel[row_range(piece), where] = picked[pl.ds(start, widths[piece - 1]), :]

    def arrive(piece, zz, yy):
        where = stripe(chip(zz, yy))
        pltpu.make_async_remote_copy(
            src_ref=block(piece, where), dst_ref=block(piece, where), send_sem=send_sem.at[0],
            recv_sem=recv_sem.at[piece, chip(zz, yy)], device_id=partner,
            device_id_type=MESH).wait_recv()

    def arrive_partner(piece):
        where = single(z, y, 1 - core)
        pltpu.make_async_remote_copy(
            src_ref=block(piece, where), dst_ref=block(piece, where), send_sem=send_sem.at[0],
            recv_sem=recv_sem.at[piece, chip(z, y)], device_id=partner,
            device_id_type=MESH).wait_recv()

    def forward(when, piece, zz, yy, target):
        where = block(piece, stripe(chip(zz, yy)))
        send(when, where, where, target, recv_sem.at[piece, chip(zz, yy)])

    down = device(z - 1, y, core)
    up = device(z + 1, y, core)
    across = device(z, 1 - y, core)

    def relay_cross(piece):
        arrive(piece, z, 1 - y)
        if balance:
            low, high = z == bottom, z == top
            if piece % 2:
                low_too, high_too = z == top - 1, z == bottom + 1
                forward(low | low_too, piece, z, 1 - y, up)
                forward(high | high_too, piece, z, 1 - y, down)
            else:
                forward(low, piece, z, 1 - y, up)
                forward(high, piece, z, 1 - y, down)

    def relay(piece, d):
        for sign in (1, -1):
            src = z + sign * d
            valid = (src <= top) if sign > 0 else (src >= bottom)
            onward = below if sign > 0 else above
            target = down if sign > 0 else up

            @pl.when(valid)
            def _():
                arrive(piece, src, y)

            forward(valid & onward, piece, src, y, target)
            cross = valid
            if balance and d == 1:
                end = (z == top - 1) if sign > 0 else (z == bottom + 1)
                cross = cross & jnp.logical_not(end)
                if piece % 2:
                    edge = (z == bottom) if sign > 0 else (z == top)
                    cross = cross & jnp.logical_not(edge)
            forward(cross, piece, src, y, across)

    def settle(piece):
        arrive_partner(piece)
        for d in range(1, depth):
            for sign in (1, -1):
                src = z + sign * d

                @pl.when((src <= top) if sign > 0 else (src >= bottom))
                def _():
                    arrive(piece, src, 1 - y)

    block_lanes = 512

    def turn(q):
        def body(i, _):
            lanes = pl.ds(pl.multiple_of(i * block_lanes, block_lanes), block_lanes)
            x = raw[q, :, lanes].astype(jnp.float32)
            rows = pl.ds(pl.multiple_of(q * quarter + i * block_lanes, block_lanes), block_lanes)
            turned[rows, :] = x.T
            return 0

        lax.fori_loop(0, quarter // block_lanes, body, 0)

    batch = lines.shape[0]

    def pick(piece):
        for h in range(2):
            first = h * half + starts[piece - 1]
            few = math.gcd(batch, widths[piece - 1])

            def body(i, _):
                base = first + i * few
                b, at = base // block_width, lax.rem(base, block_width)
                for u in range(few):
                    lines[pl.ds(u, 1), :] = turned[pl.ds(index_ref[b, at + u], 1), :]
                picked[pl.ds(pl.multiple_of(base, few), few), :] = (
                    lines[:few, :].astype(jnp.bfloat16))
                return 0

            lax.fori_loop(0, widths[piece - 1] // few, body, 0)

    lanes = here
    expr_parts = genes // lanes

    def loading_expr(p):
        return pltpu.make_async_copy(expr.at[:, pl.ds(p * lanes, lanes)], ebuf, expr_sem)

    def widen(p):
        loading_expr(p).wait()
        columns = slice(p * lanes, (p + 1) * lanes)
        step = samples // 16

        def body(i, total):
            rows = pl.ds(pl.multiple_of(i * step, step), step)
            x = ebuf[rows, :].astype(jnp.float32)
            turned[rows, :] = x
            return total + jnp.sum(x * x, axis=0, keepdims=True)

        total = lax.fori_loop(0, 16, body, jnp.zeros((1, lanes), jnp.float32))
        norm[:, columns] = jnp.broadcast_to(total, (8, lanes))
        if p + 1 < expr_parts:
            loading_expr(p + 1).start()
        else:
            send(None, norm, norm_other, partner, core_sem.at[0])

    match_parts = 4

    def match(p, q):
        columns = slice(p * lanes, (p + 1) * lanes)
        span = samples // match_parts

        def body(i, _):
            base = q * span + i * batch
            for u in range(batch):
                lines[pl.ds(u, 1), :] = turned[pl.ds(row_ref[base + u], 1), :]
            mine[pl.ds(pl.multiple_of(base, batch), batch), columns] = (
                lines[...].astype(jnp.bfloat16))
            return 0

        lax.fori_loop(0, span // batch, body, 0)

    def send_match(p, q):
        span = samples // match_parts
        where = (pl.ds(q * span, span), pl.ds(p * lanes, lanes))
        send(None, mine.at[where], theirs.at[where], partner,
             core_sem.at[1 + p * match_parts + q])

    def arrive_match():
        pltpu.make_async_remote_copy(
            src_ref=norm, dst_ref=norm_other, send_sem=send_sem.at[0],
            recv_sem=core_sem.at[0], device_id=partner, device_id_type=MESH).wait_recv()
        span = samples // match_parts
        for p in range(expr_parts):
            for q in range(match_parts):
                where = (pl.ds(q * span, span), pl.ds(p * lanes, lanes))
                pltpu.make_async_remote_copy(
                    src_ref=mine.at[where], dst_ref=theirs.at[where], send_sem=send_sem.at[0],
                    recv_sem=core_sem.at[1 + p * match_parts + q], device_id=partner,
                    device_id_type=MESH).wait_recv()

    span = min(SPAN, samples)
    spans = samples // span

    def cut(j):
        return pl.ds(pl.multiple_of(j * span, span), span)

    def make_gram():
        settle(0)
        gram[...] = jnp.zeros_like(gram)

        def add(j, _):
            c = covs[:, cut(j)]
            gram[...] += lax.dot_general(c, c, COLUMNS, preferred_element_type=jnp.float32)
            return 0

        lax.fori_loop(0, spans, add, 0)
        row = lax.broadcasted_iota(jnp.int32, (covars, covars), 0)
        lane = lax.broadcasted_iota(jnp.int32, (covars, covars), 1)
        right[...] = (row == lane).astype(jnp.float32)

    def eliminate(low, high):
        lane = lax.broadcasted_iota(jnp.int32, (covars, covars), 1)
        first_lane = lax.broadcasted_iota(jnp.int32, (1, covars), 1)
        first_row = lax.broadcasted_iota(jnp.int32, (covars, 1), 0)

        def body(i, _):
            g_row, r_row = gram[pl.ds(i, 1), :], right[pl.ds(i, 1), :]
            pivot = jnp.sum(jnp.where(first_lane == i, g_row, 0.0), axis=1, keepdims=True)
            g = gram[...]
            column = jnp.sum(jnp.where(lane == i, g, 0.0), axis=1, keepdims=True)
            factor = jnp.where(first_row > i, column / pivot, 0.0)
            lower[pl.ds(i, 1), :] = r_row
            lower_scaled[pl.ds(i, 1), :] = r_row / pivot
            gram[...] = g - factor * g_row
            right[...] = right[...] - factor * r_row
            return 0

        lax.fori_loop(low, high, body, 0)

    def solve(piece):
        settle(piece)
        rows = row_range(piece)

        def load(j, total):
            return total + lax.dot_general(
                panel[rows, cut(j)], covs[:, cut(j)], COLUMNS,
                preferred_element_type=jnp.float32)

        loads = lax.fori_loop(0, spans, load, jnp.zeros((widths[piece - 1], covars), jnp.float32))
        solved = lax.dot_general(loads, lower[...], COLUMNS, precision=lax.Precision.HIGHEST,
                                 preferred_element_type=jnp.float32)
        coeffs = jnp.dot(solved, lower_scaled[...], precision=lax.Precision.HIGHEST,
                         preferred_element_type=jnp.float32)
        parts[:widths[piece - 1], :] = jnp.concatenate(terms(coeffs), axis=1)
        sq[...] = jnp.zeros_like(sq)

    def product(piece, j):
        rows = row_range(piece)
        c = covs[:, cut(j)]
        tall = widths[piece - 1]
        fitted = jnp.dot(parts[:tall, :], jnp.concatenate([c, c, c], axis=0),
                         preferred_element_type=jnp.float32)
        resid = (panel[rows, cut(j)].astype(jnp.float32) - fitted).astype(jnp.bfloat16)
        wide = resid.astype(jnp.float32)
        sq[:tall, :] += jnp.sum(wide * wide, axis=1, keepdims=True)
        kept = jnp.dot(resid, mine[cut(j), :], preferred_element_type=jnp.float32)
        given = jnp.dot(resid, theirs[cut(j), :], preferred_element_type=jnp.float32)
        if j == 0:
            result[rows, :] = kept
            part[rows, :] = given
        else:
            result[rows, :] += kept
            part[rows, :] += given

    def out_rows(piece):
        return pl.ds(pl.multiple_of(core * half + starts[piece - 1], 16), widths[piece - 1])

    def finish(piece):
        rows = row_range(piece)
        size = scale * lax.rsqrt(sq[:widths[piece - 1], :] + epsilon)
        part[rows, :] = part[rows, :] * size * lax.rsqrt(norm_other[:1, :] + epsilon)
        out_ref[out_rows(piece), :] = result[rows, :] * size * lax.rsqrt(norm[:1, :] + epsilon)

    def give(piece):
        send(None, part.at[row_range(piece), :], out_ref.at[out_rows(piece), :], partner,
             core_sem.at[1 + expr_parts * match_parts + piece - 1])

    def receive(piece):
        rows = pl.ds(pl.multiple_of((1 - core) * half + starts[piece - 1], 16), widths[piece - 1])
        pltpu.make_async_remote_copy(
            src_ref=part.at[row_range(piece), :], dst_ref=out_ref.at[rows, :],
            send_sem=send_sem.at[0],
            recv_sem=core_sem.at[1 + expr_parts * match_parts + piece - 1], device_id=partner,
            device_id_type=MESH).wait_recv()

    work = []

    def todo(earliest, weight, call, *args):
        work.append((earliest, weight, functools.partial(call, *args)))

    for piece in range(3, pieces):
        todo(0, 0.6, pick, piece)
    sent = None
    for p in range(expr_parts):
        todo(0, 1.0, widen, p)
        for q in range(match_parts):
            todo(0, 1.3, match, p, q)
            if sent is not None:
                todo(0, 0.0, send_match, *sent)
            sent = (p, q)
    todo(0, 0.0, send_match, *sent)
    todo(depth - 1, 0.7, make_gram)
    rounds = covars // 12
    for i in range(12):
        todo(depth - 1, 1.2, eliminate, i * rounds,
             covars if i == 11 else (i + 1) * rounds)
    todo(1, 0.0, arrive_match)
    for piece in range(1, pieces):
        share = widths[piece - 1] * len(widths) / half
        todo(piece + depth - 1, 0.3 + 0.3 * share, solve, piece)
        for j in range(spans):
            todo(piece + depth - 1, 0.2 + 0.3 * share, product, piece, j)
        todo(piece + depth - 1, 0.3 * share, finish, piece)
        todo(piece + depth - 1, 0.0, give, piece)

    pl.semaphore_wait(barrier, 3 + 2 * below.astype(jnp.int32) + 2 * above.astype(jnp.int32))
    send_own(0)
    for q in range(quarters):
        loading(q).wait()
        turn(q)
    loading_expr(0).start()
    pick(1)
    pick(2)
    send_own(1)
    send_own(2)
    steps = pieces + depth - 2
    marks, released = [], [0]

    def release(end):
        for when, copy in started[released[0]:end]:
            if when is None:
                copy.wait_send()
            else:
                pl.when(when)(copy.wait_send)
        released[0] = max(end, released[0])


    for step in range(steps):
        if 0 < step and step + 2 < pieces:
            send_own(step + 2)
        left = sum(w for e, w, _ in work if e < steps)
        quota = left / (steps - step) / depth

        def run():
            spent = 0.0
            while work and work[0][0] <= step and (spent < quota or work[0][1] == 0.0):
                spent += work[0][1]
                work.pop(0)[2]()

        if step < pieces:
            relay_cross(step)
        for d in range(1, depth):
            if 0 <= step + 1 - d < pieces:
                relay(step + 1 - d, d)
        for _ in range(depth):
            run()
        marks.append(len(started))
        if step >= 3:
            release(marks[step - 3])
    for count, (_, _, call) in enumerate(work):
        call()
        if count == 0:
            release(marks[-3])
    for piece in range(1, pieces - 1):
        receive(piece)
    release(len(started))
    receive(pieces - 1)


def local(n, dosage, covariates, expression, block_index, expr_row):
    blocks, block_width = block_index.shape
    here, covars = covariates.shape
    samples, genes = expression.shape
    variants = blocks * block_width
    half = variants // 2
    tallest = max(PATTERN) * half // sum(PATTERN)
    scale = math.sqrt(samples - covars - 1)
    vmem = pl.BlockSpec(memory_space=pltpu.VMEM)
    smem = pl.BlockSpec(memory_space=pltpu.SMEM)
    hbm = pl.BlockSpec(memory_space=pl.ANY)
    depth = n // 4
    pieces = len(PATTERN) + 1
    sends = pieces * (7 + 2 + 4 * (depth - 1)) + 64
    square = pltpu.VMEM((covars, covars), jnp.float32)
    quarters = 4
    return pl.pallas_call(
        functools.partial(exchange, n, scale),
        out_shape=jax.ShapeDtypeStruct((variants, genes), jnp.float32),
        in_specs=[hbm, vmem, hbm, smem, smem],
        out_specs=vmem,
        scratch_shapes=[
            pltpu.VMEM((half, samples), jnp.bfloat16),
            pltpu.VMEM((covars, samples), jnp.bfloat16),
            pltpu.VMEM((samples, genes), jnp.bfloat16),
            pltpu.VMEM((samples, genes), jnp.bfloat16),
            pltpu.VMEM((variants, here), jnp.bfloat16),
            pltpu.VMEM((max(dosage.shape[1], samples), here), jnp.float32),
            pltpu.VMEM((quarters, here, dosage.shape[1] // quarters), jnp.bfloat16),
            pltpu.VMEM((64, here), jnp.float32),
            pltpu.VMEM((8, 128), jnp.float32),
            pltpu.VMEM((samples, here), jnp.bfloat16),
            pltpu.VMEM((8, genes), jnp.float32),
            pltpu.VMEM((8, genes), jnp.float32),
            pltpu.VMEM((half, genes), jnp.float32),
            square, square, square, square,
            pltpu.VMEM((tallest, 3 * covars), jnp.bfloat16),
            pltpu.VMEM((tallest, 1), jnp.float32),
            pltpu.VMEM((half, genes), jnp.float32),
            pltpu.SemaphoreType.DMA((quarters,)),
            pltpu.SemaphoreType.DMA,
            pltpu.SemaphoreType.DMA((sends,)),
            pltpu.SemaphoreType.DMA((pieces, n // 2)),
            pltpu.SemaphoreType.DMA((64,)),
        ],
        compiler_params=pltpu.CompilerParams(
            collective_id=0, has_side_effects=True, vmem_limit_bytes=63 * 2**20),
    )(dosage, covariates.T, expression, block_index, expr_row)


def solution(mesh):
    placed = (
        P(("groups", "samp"), None),
        P(("groups", "samp"), None),
        P("groups", "samp"),
        P("groups", None),
        P("groups"),
    )
    return jax.shard_map(
        functools.partial(local, mesh.shape["samp"]),
        mesh=mesh, in_specs=placed, out_specs=P("groups", "samp"), check_vma=False
    )
```
